32 devices in a mesh: seq: 16 (over z, x, core), chan: 2 (over y).
Axes of the slice: x: 2, y: 2, z: 4, core: 2. Of those that a mesh axis runs over, the one named last changes fastest.
Arguments:
- gate_input: bfloat16 [1024, 4096], P('seq', 'chan'), may hold values from -6 to 6
- key_input: bfloat16 [1024, 4096], P('seq', 'chan'), may hold values from -6 to 6
- value_input: bfloat16 [1024, 4096], P('seq', 'chan'), may hold values from -6 to 6
- decay_rate: float32 [16, 4096], P(None, 'chan'), may hold values from 0.0009765625 to 0.1
- residue: float32 [16, 4096], P(None, 'chan'), may hold values from -1.5 to 1.5
- skip_gain: float32 [4096], P('chan'), may hold values from -3 to 3
- out_weight: bfloat16 [4096, 4096], P('chan', 'seq'), may hold values from -0.125 to 0.125
Outputs:
- mixed: bfloat16 [1024, 4096], P('seq', 'chan')
The draws below stay inside these ranges and needn't reach their ends.
All inputs are finite; a program needn't handle non-finite values.
Results may differ from the reference program's by a relative error of at most 0.014.
Values may be sent and summed in bfloat16 or wider, within the bound.
A program may use at most 64 MiB of HBM per device.

```python
import math
import jax
import jax.numpy as jnp
from jax import lax

D = 4096
MODES = 16
TOK_DEV = 64
LENGTH = 1024
N_SEQ = 16
N_CHAN = 2


def strengthened(array, own_key, source, target, blocks, factor):
    owner, partner = [(jnp.arange(array.shape[dim]) // (array.shape[dim] // blocks)).reshape([-1 if axis == dim else 1 for axis in range(array.ndim)]) for dim in (source, target)]
    chosen = jax.random.permutation(own_key, blocks)[partner]
    strong = (owner == chosen) | (owner == (partner + blocks // 2) % blocks)
    return jnp.where(strong, factor * array, array)


def block_scale(rng, extent, split, smallest, top_value):
    loudness, own = 1.0, jax.random.fold_in(rng, 6)
    for dim, shards_of in split:
        steps = jnp.exp(jax.random.uniform(jax.random.fold_in(own, dim), (shards_of,), jnp.float32, smallest / len(split), top_value / len(split)))
        loudness = loudness * jnp.repeat(steps, extent[dim] // shards_of).reshape([-1 if axis == dim else 1 for axis in range(len(extent))])
    return loudness


def gaussian(rng, dims, width, most, shards=(), dtype=jnp.bfloat16):
    drawn = width * jax.random.normal(rng, dims, jnp.float32)
    if shards:
        drawn = drawn * block_scale(rng, dims, shards, -0.22, 0.18)
    return jnp.clip(drawn, -most, most).astype(dtype)


def gaussian_with(stream_key, dims, scale, reach, cuts, heavy, dtype=jnp.bfloat16):
    values = scale * jax.random.normal(stream_key, dims, jnp.float32)
    if cuts:
        values = values * block_scale(stream_key, dims, cuts, -0.22, 0.18)
    return jnp.clip(strengthened(values, jax.random.fold_in(stream_key, 3), *heavy), -reach, reach).astype(dtype)


def setup_inputs(seed: int = 0) -> dict:
    splits = jax.random.split(jax.random.key(seed), 8)
    return {
        "gate_input": gaussian(splits[0], (LENGTH, D), 1.0, 6.0, ((0, 16), (1, 2))),
        "key_input": gaussian(splits[1], (LENGTH, D), 1.0, 6.0, ((0, 16), (1, 2))),
        "value_input": gaussian(splits[2], (LENGTH, D), 1.0, 6.0, ((0, 16), (1, 2))),
        "decay_rate": jnp.clip(jnp.exp(math.log(0.1) - 4.6288867 * jax.random.uniform(splits[3], (MODES, D), jnp.float32) ** block_scale(splits[3], (MODES, D), ((1, 2),), -0.2, 0.2)), 0.0009765625, 0.1),
        "residue": gaussian(splits[4], (MODES, D), MODES ** -0.5, 1.5, ((1, 2),), jnp.float32),
        "skip_gain": gaussian(splits[5], (D,), 0.5, 3.0, ((0, 2),), jnp.float32),
        "out_weight": gaussian_with(splits[6], (D, D), D ** -0.5, 0.125, ((0, 2), (1, 16)), (0, 1, 16, 2.0)),
    }


def reference(gate_input, key_input, value_input, decay_rate, residue, skip_gain, out_weight):
    total_rows = TOK_DEV * N_SEQ
    padded_len = 2 * total_rows
    group_cols = D // N_CHAN
    signal = key_input.astype(jnp.float32) * value_input.astype(jnp.float32)
    amplitude = residue * jnp.sqrt(-jnp.expm1(-2.0 * decay_rate))
    positions = jnp.arange(total_rows).astype(jnp.float32)
    pieces = []
    for group_index in range(N_CHAN):
        first_col = group_index * group_cols
        group_signal = signal[:, first_col:first_col + group_cols]
        rates = decay_rate[:, first_col:first_col + group_cols]
        amps = amplitude[:, first_col:first_col + group_cols]

        def add_mode(mode_index, totals):
            return totals + amps[mode_index][None, :] * jnp.exp(-rates[mode_index][None, :] * positions[:, None])
        response = lax.fori_loop(0, MODES, add_mode, jnp.zeros((total_rows, group_cols), jnp.float32))
        product = jnp.fft.rfft(group_signal, n=padded_len, axis=0) * jnp.fft.rfft(response, n=padded_len, axis=0)
        pieces.append(jnp.fft.irfft(product, n=padded_len, axis=0)[:total_rows])
    convolved = jnp.concatenate(pieces, axis=1)
    gated_rows = (gate_input.astype(jnp.float32) * (convolved + skip_gain[None, :] * signal)).astype(jnp.bfloat16)
    summed = jnp.zeros((total_rows, D), jnp.float32)
    for group_index in range(N_CHAN):
        first_col = group_index * group_cols
        partial_sum = jnp.dot(gated_rows[:, first_col:first_col + group_cols].astype(jnp.float32), out_weight[first_col:first_col + group_cols].astype(jnp.float32), precision=lax.Precision.HIGHEST)
        summed = summed + partial_sum.astype(jnp.bfloat16).astype(jnp.float32)
    return summed.astype(jnp.bfloat16)
```

```python
import functools

import jax
import jax.numpy as jnp
from jax import lax
from jax.experimental import pallas as pl
from jax.experimental.pallas import tpu as pltpu
from jax.sharding import PartitionSpec as P

MESH = pl.DeviceIdType.MESH
F32 = jnp.float32
BF16 = jnp.bfloat16
LANES = 128
SUB = 8


def kernel(
    n, n_chan,
    q_ref, k_ref, v_ref, rate_ref, amp_ref, skip_ref, w_ref, out_ref,
    sig, local, padded, fades, ends, ends_all, starts_all, starts, gathered, partial, landed,
    end_send, end_recv, start_send, start_recv, gather_send, gather_recv, part_send, part_recv,
):
    tok, chans = q_ref.shape
    modes = rate_ref.shape[0]
    blocks = chans // LANES
    rows = modes * blocks // n
    per_block = modes // rows
    width = w_ref.shape[1]
    per_chan = n // n_chan
    ring = n // 4
    tiles = tok // SUB

    me = lax.axis_index("seq")
    chan = lax.axis_index("chan")
    z = me // 4
    x = (me // 2) % 2
    c = me % 2
    steps = lax.broadcasted_iota(jnp.int32, (SUB, LANES), 0).astype(F32)

    def lanes(b):
        return pl.ds(pl.multiple_of(b * LANES, LANES), LANES)

    def end_block(b, _):
        at = lanes(b)
        s = k_ref[:, at].astype(F32) * v_ref[:, at].astype(F32)
        sig[:, at] = s
        found = []
        for m in range(modes):
            rate = rate_ref[pl.ds(m, 1), at]
            jump = jnp.exp(-float(SUB) * rate)
            total = s[:SUB]
            for t in range(1, tiles):
                total = total * jump + s[t * SUB:(t + 1) * SUB]
            total = total * jnp.exp(-rate * (float(SUB - 1) - steps))
            found.append(jnp.sum(total, axis=0, keepdims=True))
        state = jnp.concatenate(found, axis=0)
        fade = jnp.exp(-float(tok) * rate_ref[:, at])
        for p in range(per_block):
            ends[b * per_block + p] = state[p * rows:(p + 1) * rows]
            fades[b * per_block + p] = fade[p * rows:(p + 1) * rows]
        return 0

    lax.fori_loop(0, blocks, end_block, 0)

    def exchange(source, target, send_sem, recv_sem):
        copies = []
        for hop in range(1, n):
            peer = lax.rem(me + hop, n)
            copy = pltpu.make_async_remote_copy(
                src_ref=source.at[peer], dst_ref=target.at[me],
                send_sem=send_sem.at[hop], recv_sem=recv_sem.at[me],
                device_id=(peer, chan), device_id_type=MESH,
            )
            copy.start()
            copies.append(copy)
        target[me] = source[me]
        return copies

    def arrivals(target, send_sem, recv_sem):
        for hop in range(1, n):
            peer = lax.rem(me + hop, n)
            pltpu.make_async_remote_copy(
                src_ref=target.at[peer], dst_ref=target.at[peer],
                send_sem=send_sem.at[hop], recv_sem=recv_sem.at[peer],
                device_id=(peer, chan), device_id_type=MESH,
            ).wait_recv()

    end_copies = exchange(ends, ends_all, end_send, end_recv)

    padded[:SUB] = jnp.zeros((SUB, LANES), F32)

    def local_block(b, _):
        at = lanes(b)
        response = [jnp.zeros((SUB, LANES), F32)] * tiles
        for m in range(modes):
            rate = rate_ref[pl.ds(m, 1), at]
            jump = jnp.exp(-float(SUB) * rate)
            term = amp_ref[pl.ds(m, 1), at] * jnp.exp(-rate * steps)
            for t in range(tiles):
                response[t] = response[t] + term
                if t < tiles - 1:
                    term = term * jump
        padded[SUB:] = jnp.concatenate(response, axis=0)
        skip = skip_ref[:, at]
        totals = [skip * sig[t * SUB:(t + 1) * SUB, at] for t in range(tiles)]
        for lag in range(SUB):
            moved = [padded[pl.ds(SUB - lag + t * SUB, SUB)] for t in range(tiles)]
            for first in range(tiles):
                value = sig[pl.ds(first * SUB + lag, 1), at]
                for t in range(first, tiles):
                    totals[t] = totals[t] + moved[t - first] * value
        for t in range(tiles):
            local[t * SUB:(t + 1) * SUB, at] = totals[t]
        return 0

    lax.fori_loop(0, blocks, local_block, 0)

    arrivals(ends_all, end_send, end_recv)
    fade = fades[me]
    state = jnp.zeros((rows, LANES), F32)
    for i in range(n):
        starts_all[i] = state
        if i < n - 1:
            state = state * fade + ends_all[i]
    start_copies = exchange(starts_all, starts, start_send, start_recv)
    arrivals(starts, start_send, start_recv)

    own_rows = pl.multiple_of(me * tok, tok)

    def gate_block(b, _):
        at = lanes(b)
        totals = [local[t * SUB:(t + 1) * SUB, at] for t in range(tiles)]
        for m in range(modes):
            rate = rate_ref[pl.ds(m, 1), at]
            jump = jnp.exp(-float(SUB) * rate)
            start = starts[b * per_block + m // rows][m % rows:m % rows + 1]
            term = (amp_ref[pl.ds(m, 1), at] * start) * jnp.exp(-rate * (steps + 1.0))
            for t in range(tiles):
                totals[t] = totals[t] + term
                if t < tiles - 1:
                    term = term * jump
        gated = q_ref[:, at].astype(F32) * jnp.concatenate(totals, axis=0)
        gathered[pl.ds(own_rows, tok), at] = gated.astype(BF16)
        return 0

    lax.fori_loop(0, blocks, gate_block, 0)

    half_rows = tok // 2
    sib = me + 1 - 2 * c
    across = me + 2 - 4 * x
    right = lax.rem(me + 4, n)
    left = lax.rem(me + n - 4, n)
    sent = []

    def slot_of(dz, dx, dc):
        return lax.rem(z + dz + ring, ring) * 4 + (x + dx - 2 * x * dx) * 2 + (c + dc - 2 * c * dc)

    def piece(half, slot):
        return gathered.at[pl.ds(pl.multiple_of(slot * tok + half * half_rows, half_rows), half_rows)]

    def send(half, slot, peer):
        copy = pltpu.make_async_remote_copy(
            src_ref=piece(half, slot), dst_ref=piece(half, slot),
            send_sem=gather_send.at[len(sent)], recv_sem=gather_recv.at[half * n + slot],
            device_id=(peer, chan), device_id_type=MESH,
        )
        copy.start()
        sent.append(copy)

    def receive(half, slot):
        pltpu.make_async_remote_copy(
            src_ref=piece(half, slot), dst_ref=piece(half, slot),
            send_sem=gather_send.at[0], recv_sem=gather_recv.at[half * n + slot],
            device_id=(sib, chan), device_id_type=MESH,
        ).wait_recv()

    def goes_on(half, d, to_right):
        far = (half == 0) == to_right
        return 2 * (d + 1) <= ring if far else 2 * (d + 1) < ring

    def pass_on(half, slot, d, go_right, go_left):
        if go_right and goes_on(half, d, True):
            send(half, slot, right)
        if go_left and goes_on(half, d, False):
            send(half, slot, left)

    out_chan = me // per_chan
    part_waits = []

    def project(dz):
        base = lax.rem(z + dz + ring, ring) * 4
        at = pl.ds(pl.multiple_of(base * tok, 4 * tok), 4 * tok)
        partial[at] = jnp.dot(
            gathered[at], w_ref[...], preferred_element_type=F32
        ).astype(BF16)
        for q in range(4):
            to = base + q
            source = partial.at[pl.ds(pl.multiple_of(to * tok, tok), tok)]
            slot = chan * per_chan + lax.rem(me, per_chan)
            copy = pltpu.make_async_remote_copy(
                src_ref=source, dst_ref=landed.at[slot],
                send_sem=part_send.at[len(part_waits)], recv_sem=part_recv.at[slot],
                device_id=(to, out_chan), device_id_type=MESH,
            )
            here = None
            if dz == 0:
                here = jnp.logical_and(to == me, out_chan == chan)

                @pl.when(here)
                def _():
                    pltpu.make_async_copy(source, landed.at[slot], part_recv.at[slot]).start()

                @pl.when(jnp.logical_not(here))
                def _():
                    copy.start()
            else:
                copy.start()
            part_waits.append((here, copy))

    send(0, me, across)
    pass_on(1, me, 0, True, True)
    pass_on(0, me, 0, True, True)
    send(1, me, across)
    for half in range(2):
        send(half, me, sib)
    other = slot_of(0, 1, 0)
    receive(0, other)
    pass_on(0, other, 0, True, True)
    send(0, other, sib)
    receive(1, other)
    send(1, other, sib)
    for half in range(2):
        for dx in range(2):
            receive(half, slot_of(0, dx, 1))
    project(0)
    d = 1
    while 2 * d <= ring:
        planes = []
        for to_right in (True, False):
            dz = -d if to_right else d
            for half in range(2):
                if not goes_on(half, d - 1, to_right):
                    continue
                for dx in range(2 if half == 0 else 1):
                    slot = slot_of(dz, dx, 0)
                    receive(half, slot)
                    pass_on(half, slot, d, to_right, not to_right)
                    if half == 1:
                        send(1, slot, across)
                    send(half, slot, sib)
            if not planes or 2 * d < ring:
                planes.append(dz)
        for dz in planes:
            slot = slot_of(dz, 1, 0)
            receive(1, slot)
            send(1, slot, sib)
        for dz in planes:
            for half in range(2):
                for dx in range(2):
                    receive(half, slot_of(dz, dx, 1))
            project(dz)
        d += 1

    for i in range(per_chan):
        total = None
        for j in range(n_chan):
            slot = j * per_chan + i
            pltpu.make_async_remote_copy(
                src_ref=landed.at[slot], dst_ref=landed.at[slot],
                send_sem=part_send.at[0], recv_sem=part_recv.at[slot],
                device_id=(sib, chan), device_id_type=MESH,
            ).wait_recv()
            part = landed[slot].astype(F32)
            total = part if total is None else total + part
        out_ref[:, i * width:(i + 1) * width] = total.astype(BF16)

    for copy in end_copies + start_copies + sent:
        copy.wait_send()
    for here, copy in part_waits:
        if here is None:
            copy.wait_send()
        else:
            @pl.when(jnp.logical_not(here))
            def _():
                copy.wait_send()


def solution(mesh):
    n, n_chan = mesh.shape["seq"], mesh.shape["chan"]
    assert n % 4 == 0 and n % n_chan == 0

    def body(gate_input, key_input, value_input, decay_rate, residue, skip_gain, out_weight):
        tok, chans = gate_input.shape
        modes = decay_rate.shape[0]
        width = out_weight.shape[1]
        rows = modes * chans // (LANES * n)
        amplitude = residue * jnp.sqrt(-jnp.expm1(-2.0 * decay_rate))
        vmem = pl.BlockSpec(memory_space=pltpu.VMEM)
        dma = pltpu.SemaphoreType.DMA
        states = pltpu.VMEM((n, rows, LANES), F32)
        return pl.pallas_call(
            functools.partial(kernel, n, n_chan),
            out_shape=jax.ShapeDtypeStruct((tok, width * (n // n_chan)), BF16),
            in_specs=[vmem] * 7,
            out_specs=vmem,
            scratch_shapes=[
                pltpu.VMEM((tok, chans), F32),
                pltpu.VMEM((tok, chans), F32),
                pltpu.VMEM((tok + SUB, LANES), F32),
                states, states, states, states, states,
                pltpu.VMEM((n * tok, chans), BF16),
                pltpu.VMEM((n * tok, width), BF16),
                pltpu.VMEM((n, tok, width), BF16),
                dma((n,)), dma((n,)), dma((n,)), dma((n,)),
                dma((8 * n,)), dma((2 * n,)), dma((n,)), dma((n,)),
            ],
            compiler_params=pltpu.CompilerParams(
                has_side_effects=True, vmem_limit_bytes=48 * 1024 * 1024
            ),
            cost_estimate=pl.CostEstimate(
                flops=2 * n * tok * chans * width, bytes_accessed=4 * tok * chans, transcendentals=0
            ),
        )(gate_input, key_input, value_input, decay_rate, amplitude,
          skip_gain.reshape(1, chans), out_weight)

    return jax.shard_map(
        body,
        mesh=mesh,
        in_specs=(
            P("seq", "chan"),
            P("seq", "chan"),
            P("seq", "chan"),
            P(None, "chan"),
            P(None, "chan"),
            P("chan"),
            P("chan", "seq"),
        ),
        out_specs=P("seq", "chan"),
        check_vma=False,
    )
```

```python
import functools

import jax
import jax.numpy as jnp
from jax import lax
from jax.experimental import pallas as pl
from jax.experimental.pallas import tpu as pltpu
from jax.sharding import PartitionSpec as P

MESH = pl.DeviceIdType.MESH
F32 = jnp.float32
BF16 = jnp.bfloat16
LANES = 128
SUB = 8


def one_minus_exp(y):
    series = jnp.ones_like(y)
    for order in range(10, 1, -1):
        series = 1.0 - y * (1.0 / order) * series
    return jnp.where(y < 0.4, y * series, 1.0 - jnp.exp(-y))


def kernel(
    n, n_chan,
    q_hbm, k_hbm, v_hbm, rate_hbm, residue_hbm, skip_ref, w_hbm, out_ref,
    q_ref, k_ref, v_ref, rate_ref, amp_ref, w_ref, w_other, load_sem, w_send, w_recv,
    sig, local, padded, fades, ends, ends_all, starts_all, starts, gathered, partial, landed,
    end_send, end_recv, start_send, start_recv, gather_send, gather_recv, part_send, part_recv,
):
    loads = [
        pltpu.make_async_copy(source, target, load_sem.at[i])
        for i, (source, target) in enumerate([
            (k_hbm, k_ref), (v_hbm, v_ref), (rate_hbm, rate_ref),
            (residue_hbm, amp_ref), (q_hbm, q_ref), (w_hbm, w_ref),
        ])
    ]
    for load in loads:
        load.start()
    tok, chans = q_ref.shape
    modes = rate_ref.shape[0]
    blocks = chans // LANES
    rows = modes * blocks // n
    per_block = modes // rows
    width = w_ref.shape[1]
    per_chan = n // n_chan
    line = n // 4
    tiles = tok // SUB

    me = lax.axis_index("seq")
    chan = lax.axis_index("chan")
    z = me // 4
    x = (me // 2) % 2
    c = me % 2
    barrier = pltpu.get_barrier_semaphore()
    for hop in range(1, n):
        pl.semaphore_signal(
            barrier, inc=1, device_id=(lax.rem(me + hop, n), chan), device_id_type=MESH
        )
    for turn in range(1, n_chan):
        for slot in range(2 * line):
            peer = (slot // 2) * 4 + x * 2 + slot % 2
            pl.semaphore_signal(
                barrier, inc=1, device_id=(peer, lax.rem(chan + turn, n_chan)), device_id_type=MESH
            )
    steps = lax.broadcasted_iota(jnp.int32, (SUB, LANES), 0).astype(F32)

    def lanes(b):
        return pl.ds(pl.multiple_of(b * LANES, LANES), LANES)

    for load in loads[:3]:
        load.wait()

    def end_block(b, _):
        at = lanes(b)
        s = k_ref[:, at].astype(F32) * v_ref[:, at].astype(F32)
        sig[:, at] = s
        found = []
        for m in range(modes):
            rate = rate_ref[pl.ds(m, 1), at]
            jump = jnp.exp(-float(SUB) * rate)
            total = s[:SUB]
            for t in range(1, tiles):
                total = total * jump + s[t * SUB:(t + 1) * SUB]
            total = total * jnp.exp(-rate * (float(SUB - 1) - steps))
            found.append(jnp.sum(total, axis=0, keepdims=True))
        state = jnp.concatenate(found, axis=0)
        fade = jnp.exp(-float(tok) * rate_ref[:, at])
        for p in range(per_block):
            ends[b * per_block + p] = state[p * rows:(p + 1) * rows]
            fades[b * per_block + p] = fade[p * rows:(p + 1) * rows]
        return 0

    lax.fori_loop(0, blocks, end_block, 0)

    pl.semaphore_wait(barrier, n - 1 + (n_chan - 1) * 2 * line)

    def exchange(source, target, send_sem, recv_sem):
        copies = []
        for hop in range(1, n):
            peer = lax.rem(me + hop, n)
            copy = pltpu.make_async_remote_copy(
                src_ref=source.at[peer], dst_ref=target.at[me],
                send_sem=send_sem.at[hop], recv_sem=recv_sem.at[me],
                device_id=(peer, chan), device_id_type=MESH,
            )
            copy.start()
            copies.append(copy)
        target[me] = source[me]
        return copies

    def arrivals(target, send_sem, recv_sem):
        for hop in range(1, n):
            peer = lax.rem(me + hop, n)
            pltpu.make_async_remote_copy(
                src_ref=target.at[peer], dst_ref=target.at[peer],
                send_sem=send_sem.at[hop], recv_sem=recv_sem.at[peer],
                device_id=(peer, chan), device_id_type=MESH,
            ).wait_recv()

    end_copies = exchange(ends, ends_all, end_send, end_recv)

    loads[3].wait()
    amp_ref[...] = amp_ref[...] * jnp.sqrt(one_minus_exp(2.0 * rate_ref[...]))

    padded[:SUB] = jnp.zeros((SUB, LANES), F32)

    def local_block(b, _):
        at = lanes(b)
        response = [jnp.zeros((SUB, LANES), F32)] * tiles
        for m in range(modes):
            rate = rate_ref[pl.ds(m, 1), at]
            jump = jnp.exp(-float(SUB) * rate)
            term = amp_ref[pl.ds(m, 1), at] * jnp.exp(-rate * steps)
            for t in range(tiles):
                response[t] = response[t] + term
                if t < tiles - 1:
                    term = term * jump
        padded[SUB:] = jnp.concatenate(response, axis=0)
        skip = skip_ref[:, at]
        totals = [skip * sig[t * SUB:(t + 1) * SUB, at] for t in range(tiles)]
        for lag in range(SUB):
            moved = [padded[pl.ds(SUB - lag + t * SUB, SUB)] for t in range(tiles)]
            for first in range(tiles):
                value = sig[pl.ds(first * SUB + lag, 1), at]
                for t in range(first, tiles):
                    totals[t] = totals[t] + moved[t - first] * value
        for t in range(tiles):
            local[t * SUB:(t + 1) * SUB, at] = totals[t]
        return 0

    lax.fori_loop(0, blocks, local_block, 0)

    arrivals(ends_all, end_send, end_recv)
    fade = fades[me]
    state = jnp.zeros((rows, LANES), F32)
    for i in range(n):
        starts_all[i] = state
        if i < n - 1:
            state = state * fade + ends_all[i]
    start_copies = exchange(starts_all, starts, start_send, start_recv)
    across = me + 2 - 4 * x
    w_copies = []
    w_rows = chans // 2
    for half in range(2):
        at = pl.ds(half * w_rows, w_rows)
        copy = pltpu.make_async_remote_copy(
            src_ref=w_hbm.at[at], dst_ref=w_other.at[at],
            send_sem=w_send.at[half], recv_sem=w_recv.at[half],
            device_id=(across, chan), device_id_type=MESH,
        )
        copy.start()
        w_copies.append(copy)
    loads[4].wait()
    arrivals(starts, start_send, start_recv)

    own_rows = pl.multiple_of((2 * z + c) * tok, tok)

    def gate_block(b, _):
        at = lanes(b)
        totals = [local[t * SUB:(t + 1) * SUB, at] for t in range(tiles)]
        for m in range(modes):
            rate = rate_ref[pl.ds(m, 1), at]
            jump = jnp.exp(-float(SUB) * rate)
            start = starts[b * per_block + m // rows][m % rows:m % rows + 1]
            term = (amp_ref[pl.ds(m, 1), at] * start) * jnp.exp(-rate * (steps + 1.0))
            for t in range(tiles):
                totals[t] = totals[t] + term
                if t < tiles - 1:
                    term = term * jump
        gated = q_ref[:, at].astype(F32) * jnp.concatenate(totals, axis=0)
        gathered[pl.ds(own_rows, tok), at] = gated.astype(BF16)
        return 0

    lax.fori_loop(0, blocks, gate_block, 0)

    half_rows = tok // 2
    sib = me + 1 - 2 * c
    has_right = z < line - 1
    has_left = z > 0
    sent = []

    def piece(half, slot):
        return gathered.at[pl.ds(pl.multiple_of(slot * tok + half * half_rows, half_rows), half_rows)]

    def send(half, slot, peer, cond):
        copy = pltpu.make_async_remote_copy(
            src_ref=piece(half, slot), dst_ref=piece(half, slot),
            send_sem=gather_send.at[len(sent)], recv_sem=gather_recv.at[half * 2 * line + slot],
            device_id=(peer, chan), device_id_type=MESH,
        )
        sent.append((cond, copy))
        pl.when(cond)(copy.start)

    def receive(half, slot):
        pltpu.make_async_remote_copy(
            src_ref=piece(half, slot), dst_ref=piece(half, slot),
            send_sem=gather_send.at[0], recv_sem=gather_recv.at[half * 2 * line + slot],
            device_id=(sib, chan), device_id_type=MESH,
        ).wait_recv()

    out_chan = me // per_chan

    def part_copy(other, zz, to_core):
        to = zz * 4 + x * 2 + to_core
        owner = across if other else me
        slot = 2 * zz + to_core
        place = chan * per_chan + lax.rem(owner, per_chan)
        source = partial.at[
            pl.ds(pl.multiple_of((other * 2 * line + slot) * tok, tok), tok)
        ]
        remote = pltpu.make_async_remote_copy(
            src_ref=source, dst_ref=landed.at[place],
            send_sem=part_send.at[other * 2 * line + slot], recv_sem=part_recv.at[place],
            device_id=(to, out_chan), device_id_type=MESH,
        )
        here = pltpu.make_async_copy(source, landed.at[place], part_recv.at[place])
        return to, remote, here

    def project(zz, other):
        at = pl.ds(pl.multiple_of(zz * 2 * tok, 2 * tok), 2 * tok)
        to_rows = pl.ds(pl.multiple_of((other * line + zz) * 2 * tok, 2 * tok), 2 * tok)
        weights = w_other if other else w_ref
        partial[to_rows] = jnp.dot(
            gathered[at], weights[...], preferred_element_type=F32
        ).astype(BF16)
        for to_core in range(2):
            to, remote, here = part_copy(other, zz, to_core)
            stays = jnp.logical_and(to == me, out_chan == chan)
            pl.when(stays)(here.start)
            pl.when(jnp.logical_not(stays))(remote.start)

    for half in range(2):
        send(half, 2 * z + c, me + 4, has_right)
        send(half, 2 * z + c, me - 4, has_left)
    for half in range(2):
        send(half, 2 * z + c, sib, z >= 0)
    loads[5].wait()
    for half in range(2):
        receive(half, 2 * z + 1 - c)
    project(z, 0)

    def others(last):
        for copy in w_copies:
            copy.wait_recv()
        project(z, 1)
        for d in range(1, last):
            for sign in (-1, 1):
                zz = z + sign * d
                there = zz >= 0 if sign < 0 else zz < line

                @pl.when(there)
                def _():
                    project(zz, 1)

    for d in range(1, line):
        if d == line - 1:
            others(d)
        for half in range(2):
            for sign in (-1, 1):
                zz = z + sign * d
                there = zz >= 0 if sign < 0 else zz < line
                onward = has_right if sign < 0 else has_left
                slot = 2 * zz + c

                @pl.when(there)
                def _():
                    receive(half, slot)

                send(half, slot, me - 4 * sign, jnp.logical_and(there, onward))
                send(half, slot, sib, there)
        for sign in (-1, 1):
            zz = z + sign * d
            there = zz >= 0 if sign < 0 else zz < line

            @pl.when(there)
            def _():
                for half in range(2):
                    receive(half, 2 * zz + 1 - c)
                project(zz, 0)
                if d == line - 1:
                    project(zz, 1)
    if line == 1:
        others(1)

    for i in range(per_chan):
        total = None
        for j in range(n_chan):
            slot = j * per_chan + i
            pltpu.make_async_remote_copy(
                src_ref=landed.at[slot], dst_ref=landed.at[slot],
                send_sem=part_send.at[0], recv_sem=part_recv.at[slot],
                device_id=(sib, chan), device_id_type=MESH,
            ).wait_recv()
            part = landed[slot].astype(F32)
            total = part if total is None else total + part
        out_ref[:, i * width:(i + 1) * width] = total.astype(BF16)

    for copy in end_copies + start_copies + w_copies:
        copy.wait_send()
    for cond, copy in sent:
        pl.when(cond)(copy.wait_send)
    for other in range(2):
        for slot in range(2 * line):
            to, remote, _ = part_copy(other, slot // 2, slot % 2)
            stays = jnp.logical_and(to == me, out_chan == chan)
            pl.when(jnp.logical_not(stays))(remote.wait_send)


def solution(mesh):
    n, n_chan = mesh.shape["seq"], mesh.shape["chan"]
    assert n % 4 == 0 and n % (4 * n_chan) == 0

    def body(gate_input, key_input, value_input, decay_rate, residue, skip_gain, out_weight):
        tok, chans = gate_input.shape
        modes = decay_rate.shape[0]
        width = out_weight.shape[1]
        rows = modes * chans // (LANES * n)
        hbm = pl.BlockSpec(memory_space=pltpu.HBM)
        vmem = pl.BlockSpec(memory_space=pltpu.VMEM)
        dma = pltpu.SemaphoreType.DMA
        states = pltpu.VMEM((n, rows, LANES), F32)
        return pl.pallas_call(
            functools.partial(kernel, n, n_chan),
            out_shape=jax.ShapeDtypeStruct((tok, width * (n // n_chan)), BF16),
            in_specs=[hbm] * 5 + [vmem, hbm],
            out_specs=vmem,
            scratch_shapes=[
                pltpu.VMEM((tok, chans), BF16),
                pltpu.VMEM((tok, chans), BF16),
                pltpu.VMEM((tok, chans), BF16),
                pltpu.VMEM((modes, chans), F32),
                pltpu.VMEM((modes, chans), F32),
                pltpu.VMEM((chans, width), BF16),
                pltpu.VMEM((chans, width), BF16),
                dma((6,)), dma((2,)), dma((2,)),
                pltpu.VMEM((tok, chans), F32),
                pltpu.VMEM((tok, chans), F32),
                pltpu.VMEM((tok + SUB, LANES), F32),
                states, states, states, states, states,
                pltpu.VMEM((n * tok // 2, chans), BF16),
                pltpu.VMEM((n * tok, width), BF16),
                pltpu.VMEM((n, tok, width), BF16),
                dma((n,)), dma((n,)), dma((n,)), dma((n,)),
                dma((2 * n,)), dma((n,)), dma((n,)), dma((n,)),
            ],
            compiler_params=pltpu.CompilerParams(
                collective_id=0, has_side_effects=True, vmem_limit_bytes=48 * 1024 * 1024
            ),
            cost_estimate=pl.CostEstimate(
                flops=2 * n * tok * chans * width, bytes_accessed=4 * tok * chans, transcendentals=0
            ),
        )(gate_input, key_input, value_input, decay_rate, residue,
          skip_gain.reshape(1, chans), out_weight)

    return jax.shard_map(
        body,
        mesh=mesh,
        in_specs=(
            P("seq", "chan"),
            P("seq", "chan"),
            P("seq", "chan"),
            P(None, "chan"),
            P(None, "chan"),
            P("chan"),
            P("chan", "seq"),
        ),
        out_specs=P("seq", "chan"),
        check_vma=False,
    )
```

```python
import functools

import jax
import jax.numpy as jnp
from jax import lax
from jax.experimental import pallas as pl
from jax.experimental.pallas import tpu as pltpu
from jax.sharding import PartitionSpec as P

MESH = pl.DeviceIdType.MESH
F32 = jnp.float32
BF16 = jnp.bfloat16
LANES = 128
SUB = 8


def one_minus_exp(y):
    series = jnp.ones_like(y)
    for order in range(10, 1, -1):
        series = 1.0 - y * (1.0 / order) * series
    return jnp.where(y < 0.4, y * series, 1.0 - jnp.exp(-y))


def kernel(
    n, n_chan,
    q_hbm, k_hbm, v_hbm, rate_hbm, residue_hbm, skip_ref, w_hbm, out_ref,
    q_ref, k_ref, v_ref, rate_ref, amp_ref, w_ref, w_other, load_sem, w_send, w_recv,
    sig, local, padded, fades, ends, ends_all, starts_all, starts, gathered, partial, landed,
    end_send, end_recv, start_send, start_recv, gather_send, gather_recv, part_send, part_recv,
):
    loads = [
        pltpu.make_async_copy(source, target, load_sem.at[i])
        for i, (source, target) in enumerate([
            (k_hbm, k_ref), (v_hbm, v_ref), (rate_hbm, rate_ref),
            (residue_hbm, amp_ref), (q_hbm, q_ref), (w_hbm, w_ref),
        ])
    ]
    for load in loads:
        load.start()
    tok, chans = q_ref.shape
    modes = rate_ref.shape[0]
    blocks = chans // LANES
    rows = modes * blocks // n
    per_block = modes // rows
    width = w_ref.shape[1]
    per_chan = n // n_chan
    line = n // 4
    tiles = tok // SUB

    me = lax.axis_index("seq")
    chan = lax.axis_index("chan")
    z = me // 4
    x = (me // 2) % 2
    c = me % 2
    barrier = pltpu.get_barrier_semaphore()
    for hop in range(1, n):
        pl.semaphore_signal(
            barrier, inc=1, device_id=(lax.rem(me + hop, n), chan), device_id_type=MESH
        )
    for turn in range(1, n_chan):
        for slot in range(2 * line):
            peer = (slot // 2) * 4 + x * 2 + slot % 2
            pl.semaphore_signal(
                barrier, inc=1, device_id=(peer, lax.rem(chan + turn, n_chan)), device_id_type=MESH
            )
    steps = lax.broadcasted_iota(jnp.int32, (SUB, LANES), 0).astype(F32)

    def lanes(b):
        return pl.ds(pl.multiple_of(b * LANES, LANES), LANES)

    for load in loads[:3]:
        load.wait()

    def end_block(b, _):
        at = lanes(b)
        s = k_ref[:, at].astype(F32) * v_ref[:, at].astype(F32)
        sig[:, at] = s
        found = []
        for m in range(modes):
            rate = rate_ref[pl.ds(m, 1), at]
            jump = jnp.exp(-float(SUB) * rate)
            total = s[:SUB]
            for t in range(1, tiles):
                total = total * jump + s[t * SUB:(t + 1) * SUB]
            total = total * jnp.exp(-rate * (float(SUB - 1) - steps))
            found.append(jnp.sum(total, axis=0, keepdims=True))
        state = jnp.concatenate(found, axis=0)
        fade = jnp.exp(-float(tok) * rate_ref[:, at])
        for p in range(per_block):
            ends[b * per_block + p] = state[p * rows:(p + 1) * rows].astype(BF16)
            fades[b * per_block + p] = fade[p * rows:(p + 1) * rows]
        return 0

    lax.fori_loop(0, blocks, end_block, 0)

    pl.semaphore_wait(barrier, n - 1 + (n_chan - 1) * 2 * line)

    def exchange(source, target, send_sem, recv_sem):
        copies = []
        for hop in range(1, n):
            peer = lax.rem(me + hop, n)
            copy = pltpu.make_async_remote_copy(
                src_ref=source.at[peer], dst_ref=target.at[me],
                send_sem=send_sem.at[hop], recv_sem=recv_sem.at[me],
                device_id=(peer, chan), device_id_type=MESH,
            )
            copy.start()
            copies.append(copy)
        target[me] = source[me]
        return copies

    def arrivals(target, send_sem, recv_sem):
        for hop in range(1, n):
            peer = lax.rem(me + hop, n)
            pltpu.make_async_remote_copy(
                src_ref=target.at[peer], dst_ref=target.at[peer],
                send_sem=send_sem.at[hop], recv_sem=recv_sem.at[peer],
                device_id=(peer, chan), device_id_type=MESH,
            ).wait_recv()

    across = me + 2 - 4 * x
    w_copies = []
    w_rows = chans // 8

    def swap(first, last):
        for part in range(first, last):
            at = pl.ds(part * w_rows, w_rows)
            copy = pltpu.make_async_remote_copy(
                src_ref=w_hbm.at[at], dst_ref=w_other.at[at],
                send_sem=w_send.at[part], recv_sem=w_recv.at[part],
                device_id=(across, chan), device_id_type=MESH,
            )
            copy.start()
            w_copies.append(copy)

    end_copies = exchange(ends, ends_all, end_send, end_recv)
    swap(0, 1)

    loads[3].wait()
    amp_ref[...] = amp_ref[...] * jnp.sqrt(one_minus_exp(2.0 * rate_ref[...]))

    padded[:SUB] = jnp.zeros((SUB, LANES), F32)

    def local_block(b, _):
        at = lanes(b)
        response = [jnp.zeros((SUB, LANES), F32)] * tiles
        for m in range(modes):
            rate = rate_ref[pl.ds(m, 1), at]
            jump = jnp.exp(-float(SUB) * rate)
            term = amp_ref[pl.ds(m, 1), at] * jnp.exp(-rate * steps)
            for t in range(tiles):
                response[t] = response[t] + term
                if t < tiles - 1:
                    term = term * jump
        padded[SUB:] = jnp.concatenate(response, axis=0)
        skip = skip_ref[:, at]
        totals = [skip * sig[t * SUB:(t + 1) * SUB, at] for t in range(tiles)]
        for lag in range(SUB):
            moved = [padded[pl.ds(SUB - lag + t * SUB, SUB)] for t in range(tiles)]
            for first in range(tiles):
                value = sig[pl.ds(first * SUB + lag, 1), at]
                for t in range(first, tiles):
                    totals[t] = totals[t] + moved[t - first] * value
        for t in range(tiles):
            local[t * SUB:(t + 1) * SUB, at] = totals[t]
        return 0

    lax.fori_loop(0, blocks, local_block, 0)

    arrivals(ends_all, end_send, end_recv)
    fade = fades[me]
    state = jnp.zeros((rows, LANES), F32)
    for i in range(n):
        starts_all[i] = state.astype(BF16)
        if i < n - 1:
            state = state * fade + ends_all[i].astype(F32)
    start_copies = exchange(starts_all, starts, start_send, start_recv)
    swap(1, 8)
    loads[4].wait()
    arrivals(starts, start_send, start_recv)

    own_rows = pl.multiple_of((2 * z + c) * tok, tok)

    def gate_block(b, _):
        at = lanes(b)
        held = [starts[b * per_block + p].astype(F32) for p in range(per_block)]
        totals = [local[t * SUB:(t + 1) * SUB, at] for t in range(tiles)]
        for m in range(modes):
            rate = rate_ref[pl.ds(m, 1), at]
            jump = jnp.exp(-float(SUB) * rate)
            start = held[m // rows][m % rows:m % rows + 1]
            term = (amp_ref[pl.ds(m, 1), at] * start) * jnp.exp(-rate * (steps + 1.0))
            for t in range(tiles):
                totals[t] = totals[t] + term
                if t < tiles - 1:
                    term = term * jump
        gated = q_ref[:, at].astype(F32) * jnp.concatenate(totals, axis=0)
        gathered[pl.ds(own_rows, tok), at] = gated.astype(BF16)
        return 0


    half_cols = chans // 2
    sib = me + 1 - 2 * c
    has_right = z < line - 1
    has_left = z > 0
    sent = []

    def piece(half, slot):
        return gathered.at[
            pl.ds(pl.multiple_of(slot * tok, tok), tok), pl.ds(half * half_cols, half_cols)
        ]

    def send(half, slot, peer, cond):
        copy = pltpu.make_async_remote_copy(
            src_ref=piece(half, slot), dst_ref=piece(half, slot),
            send_sem=gather_send.at[len(sent)], recv_sem=gather_recv.at[half * 2 * line + slot],
            device_id=(peer, chan), device_id_type=MESH,
        )
        sent.append((cond, copy))
        pl.when(cond)(copy.start)

    def receive(half, slot):
        pltpu.make_async_remote_copy(
            src_ref=piece(half, slot), dst_ref=piece(half, slot),
            send_sem=gather_send.at[0], recv_sem=gather_recv.at[half * 2 * line + slot],
            device_id=(sib, chan), device_id_type=MESH,
        ).wait_recv()

    out_chan = me // per_chan

    def part_copy(other, zz, to_core):
        to = zz * 4 + x * 2 + to_core
        owner = across if other else me
        slot = 2 * zz + to_core
        place = chan * per_chan + lax.rem(owner, per_chan)
        source = partial.at[
            pl.ds(pl.multiple_of((other * 2 * line + slot) * tok, tok), tok)
        ]
        remote = pltpu.make_async_remote_copy(
            src_ref=source, dst_ref=landed.at[place],
            send_sem=part_send.at[other * 2 * line + slot], recv_sem=part_recv.at[place],
            device_id=(to, out_chan), device_id_type=MESH,
        )
        here = pltpu.make_async_copy(source, landed.at[place], part_recv.at[place])
        return to, remote, here

    def project(zz, other):
        at = pl.ds(pl.multiple_of(zz * 2 * tok, 2 * tok), 2 * tok)
        to_rows = pl.ds(pl.multiple_of((other * line + zz) * 2 * tok, 2 * tok), 2 * tok)
        weights = w_other if other else w_ref
        partial[to_rows] = jnp.dot(
            gathered[at], weights[...], preferred_element_type=F32
        ).astype(BF16)
        for to_core in range(2):
            to, remote, here = part_copy(other, zz, to_core)
            stays = jnp.logical_and(to == me, out_chan == chan)
            pl.when(stays)(here.start)
            pl.when(jnp.logical_not(stays))(remote.start)

    for half in range(2):
        lax.fori_loop(half * blocks // 2, (half + 1) * blocks // 2, gate_block, 0)
        send(half, 2 * z + c, me + 4, has_right)
        send(half, 2 * z + c, me - 4, has_left)
        send(half, 2 * z + c, sib, z >= 0)
    loads[5].wait()
    for half in range(2):
        receive(half, 2 * z + 1 - c)
    project(z, 0)

    def others(last):
        for copy in w_copies:
            copy.wait_recv()
        project(z, 1)
        for d in range(1, last):
            for sign in (-1, 1):
                zz = z + sign * d
                there = zz >= 0 if sign < 0 else zz < line

                @pl.when(there)
                def _():
                    project(zz, 1)

    for d in range(1, line):
        if d == line - 1:
            others(d)
        for half in range(2):
            for sign in (-1, 1):
                zz = z + sign * d
                there = zz >= 0 if sign < 0 else zz < line
                onward = has_right if sign < 0 else has_left
                slot = 2 * zz + c

                @pl.when(there)
                def _():
                    receive(half, slot)

                send(half, slot, me - 4 * sign, jnp.logical_and(there, onward))
                send(half, slot, sib, there)
        for sign in (-1, 1):
            zz = z + sign * d
            there = zz >= 0 if sign < 0 else zz < line

            @pl.when(there)
            def _():
                for half in range(2):
                    receive(half, 2 * zz + 1 - c)
                project(zz, 0)
                if d == line - 1:
                    project(zz, 1)
    if line == 1:
        others(1)

    for i in range(per_chan):
        total = None
        for j in range(n_chan):
            slot = j * per_chan + i
            pltpu.make_async_remote_copy(
                src_ref=landed.at[slot], dst_ref=landed.at[slot],
                send_sem=part_send.at[0], recv_sem=part_recv.at[slot],
                device_id=(sib, chan), device_id_type=MESH,
            ).wait_recv()
            part = landed[slot].astype(F32)
            total = part if total is None else total + part
        out_ref[:, i * width:(i + 1) * width] = total.astype(BF16)

    for copy in end_copies + start_copies + w_copies:
        copy.wait_send()
    for cond, copy in sent:
        pl.when(cond)(copy.wait_send)
    for other in range(2):
        for slot in range(2 * line):
            to, remote, _ = part_copy(other, slot // 2, slot % 2)
            stays = jnp.logical_and(to == me, out_chan == chan)
            pl.when(jnp.logical_not(stays))(remote.wait_send)


def solution(mesh):
    n, n_chan = mesh.shape["seq"], mesh.shape["chan"]
    assert n % 4 == 0 and n % (4 * n_chan) == 0

    def body(gate_input, key_input, value_input, decay_rate, residue, skip_gain, out_weight):
        tok, chans = gate_input.shape
        modes = decay_rate.shape[0]
        width = out_weight.shape[1]
        rows = modes * chans // (LANES * n)
        hbm = pl.BlockSpec(memory_space=pltpu.HBM)
        vmem = pl.BlockSpec(memory_space=pltpu.VMEM)
        dma = pltpu.SemaphoreType.DMA
        states = pltpu.VMEM((n, rows, LANES), BF16)
        return pl.pallas_call(
            functools.partial(kernel, n, n_chan),
            out_shape=jax.ShapeDtypeStruct((tok, width * (n // n_chan)), BF16),
            in_specs=[hbm] * 5 + [vmem, hbm],
            out_specs=vmem,
            scratch_shapes=[
                pltpu.VMEM((tok, chans), BF16),
                pltpu.VMEM((tok, chans), BF16),
                pltpu.VMEM((tok, chans), BF16),
                pltpu.VMEM((modes, chans), F32),
                pltpu.VMEM((modes, chans), F32),
                pltpu.VMEM((chans, width), BF16),
                pltpu.VMEM((chans, width), BF16),
                dma((6,)), dma((8,)), dma((8,)),
                pltpu.VMEM((tok, chans), F32),
                pltpu.VMEM((tok, chans), F32),
                pltpu.VMEM((tok + SUB, LANES), F32),
                pltpu.VMEM((n, rows, LANES), F32),
                states, states, states, states,
                pltpu.VMEM((n * tok // 2, chans), BF16),
                pltpu.VMEM((n * tok, width), BF16),
                pltpu.VMEM((n, tok, width), BF16),
                dma((n,)), dma((n,)), dma((n,)), dma((n,)),
                dma((2 * n,)), dma((n,)), dma((n,)), dma((n,)),
            ],
            compiler_params=pltpu.CompilerParams(
                collective_id=0, has_side_effects=True, vmem_limit_bytes=67043328
            ),
            cost_estimate=pl.CostEstimate(
                flops=2 * n * tok * chans * width, bytes_accessed=4 * tok * chans, transcendentals=0
            ),
        )(gate_input, key_input, value_input, decay_rate, residue,
          skip_gain.reshape(1, chans), out_weight)

    return jax.shard_map(
        body,
        mesh=mesh,
        in_specs=(
            P("seq", "chan"),
            P("seq", "chan"),
            P("seq", "chan"),
            P(None, "chan"),
            P(None, "chan"),
            P("chan"),
            P("chan", "seq"),
        ),
        out_specs=P("seq", "chan"),
        check_vma=False,
    )
```

```python
import functools

import jax
import jax.numpy as jnp
from jax import lax
from jax.experimental import pallas as pl
from jax.experimental.pallas import tpu as pltpu
from jax.sharding import PartitionSpec as P

MESH = pl.DeviceIdType.MESH
F32 = jnp.float32
BF16 = jnp.bfloat16
LANES = 128
SUB = 8


def one_minus_exp(y):
    series = jnp.ones_like(y)
    for order in range(10, 1, -1):
        series = 1.0 - y * (1.0 / order) * series
    return jnp.where(y < 0.4, y * series, 1.0 - jnp.exp(-y))


def kernel(
    n, n_chan,
    q_hbm, k_hbm, v_hbm, rate_hbm, residue_hbm, skip_ref, w_hbm, out_ref,
    q_ref, k_ref, v_ref, rate_ref, amp_ref, w_ref, w_other, load_sem, w_send, w_recv,
    sig, local, padded, fades, ends, ends_all, starts_all, starts, gathered, partial, landed,
    end_send, end_recv, start_send, start_recv, gather_send, gather_recv, part_send, part_recv,
):
    loads = [
        pltpu.make_async_copy(source, target, load_sem.at[i])
        for i, (source, target) in enumerate([
            (k_hbm, k_ref), (v_hbm, v_ref), (rate_hbm, rate_ref),
            (residue_hbm, amp_ref), (q_hbm, q_ref), (w_hbm, w_ref),
        ])
    ]
    for load in loads:
        load.start()
    tok, chans = q_ref.shape
    modes = rate_ref.shape[0]
    blocks = chans // LANES
    rows = modes * blocks // n
    per_block = modes // rows
    width = w_ref.shape[1]
    per_chan = n // n_chan
    line = n // 4
    tiles = tok // SUB

    me = lax.axis_index("seq")
    chan = lax.axis_index("chan")
    z = me // 4
    x = (me // 2) % 2
    c = me % 2
    barrier = pltpu.get_barrier_semaphore()
    for hop in range(1, n):
        pl.semaphore_signal(
            barrier, inc=1, device_id=(lax.rem(me + hop, n), chan), device_id_type=MESH
        )
    for turn in range(1, n_chan):
        for slot in range(2 * line):
            peer = (slot // 2) * 4 + x * 2 + slot % 2
            pl.semaphore_signal(
                barrier, inc=1, device_id=(peer, lax.rem(chan + turn, n_chan)), device_id_type=MESH
            )
    steps = lax.broadcasted_iota(jnp.int32, (SUB, LANES), 0).astype(F32)

    def lanes(b):
        return pl.ds(pl.multiple_of(b * LANES, LANES), LANES)

    for load in loads[:3]:
        load.wait()

    def end_block(b, _):
        at = lanes(b)
        s = k_ref[:, at].astype(F32) * v_ref[:, at].astype(F32)
        sig[:, at] = s
        found = []
        for m in range(modes):
            rate = rate_ref[pl.ds(m, 1), at]
            jump = jnp.exp(-float(SUB) * rate)
            total = s[:SUB]
            for t in range(1, tiles):
                total = total * jump + s[t * SUB:(t + 1) * SUB]
            total = total * jnp.exp(-rate * (float(SUB - 1) - steps))
            found.append(jnp.sum(total, axis=0, keepdims=True))
        state = jnp.concatenate(found, axis=0)
        fade = jnp.exp(-float(tok) * rate_ref[:, at])
        for p in range(per_block):
            ends[b * per_block + p] = state[p * rows:(p + 1) * rows].astype(BF16)
            fades[b * per_block + p] = fade[p * rows:(p + 1) * rows]
        return 0

    lax.fori_loop(0, blocks, end_block, 0)

    pl.semaphore_wait(barrier, n - 1 + (n_chan - 1) * 2 * line)

    def exchange(source, target, send_sem, recv_sem):
        copies = []
        for hop in sorted(range(1, n), key=lambda h: abs(h - n // 2)):
            peer = lax.rem(me + hop, n)
            copy = pltpu.make_async_remote_copy(
                src_ref=source.at[peer], dst_ref=target.at[me],
                send_sem=send_sem.at[hop], recv_sem=recv_sem.at[me],
                device_id=(peer, chan), device_id_type=MESH,
            )
            copy.start()
            copies.append(copy)
        target[me] = source[me]
        return copies

    def arrivals(target, send_sem, recv_sem):
        for hop in range(1, n):
            peer = lax.rem(me + hop, n)
            pltpu.make_async_remote_copy(
                src_ref=target.at[peer], dst_ref=target.at[peer],
                send_sem=send_sem.at[hop], recv_sem=recv_sem.at[peer],
                device_id=(peer, chan), device_id_type=MESH,
            ).wait_recv()

    across = me + 2 - 4 * x
    w_copies = []
    w_rows = chans // 8

    def swap(first, last):
        for part in range(first, last):
            at = pl.ds(part * w_rows, w_rows)
            copy = pltpu.make_async_remote_copy(
                src_ref=w_hbm.at[at], dst_ref=w_other.at[at],
                send_sem=w_send.at[part], recv_sem=w_recv.at[part],
                device_id=(across, chan), device_id_type=MESH,
            )
            copy.start()
            w_copies.append(copy)

    end_copies = exchange(ends, ends_all, end_send, end_recv)
    swap(0, 1)

    loads[3].wait()
    amp_ref[...] = amp_ref[...] * jnp.sqrt(one_minus_exp(2.0 * rate_ref[...]))

    padded[:SUB] = jnp.zeros((SUB, LANES), F32)

    def local_block(b, _):
        at = lanes(b)
        response = [jnp.zeros((SUB, LANES), F32)] * tiles
        for m in range(modes):
            rate = rate_ref[pl.ds(m, 1), at]
            jump = jnp.exp(-float(SUB) * rate)
            term = amp_ref[pl.ds(m, 1), at] * jnp.exp(-rate * steps)
            for t in range(tiles):
                response[t] = response[t] + term
                if t < tiles - 1:
                    term = term * jump
        padded[SUB:] = jnp.concatenate(response, axis=0)
        skip = skip_ref[:, at]
        totals = [skip * sig[t * SUB:(t + 1) * SUB, at] for t in range(tiles)]
        for lag in range(SUB):
            moved = [padded[pl.ds(SUB - lag + t * SUB, SUB)] for t in range(tiles)]
            for first in range(tiles):
                value = sig[pl.ds(first * SUB + lag, 1), at]
                for t in range(first, tiles):
                    totals[t] = totals[t] + moved[t - first] * value
        for t in range(tiles):
            local[t * SUB:(t + 1) * SUB, at] = totals[t]
        return 0

    lax.fori_loop(0, blocks, local_block, 0)

    arrivals(ends_all, end_send, end_recv)
    fade = fades[me]
    state = jnp.zeros((rows, LANES), F32)
    for i in range(n):
        starts_all[i] = state.astype(BF16)
        if i < n - 1:
            state = state * fade + ends_all[i].astype(F32)
    start_copies = exchange(starts_all, starts, start_send, start_recv)
    swap(1, 8)
    loads[4].wait()
    arrivals(starts, start_send, start_recv)

    own_rows = pl.multiple_of((2 * z + c) * tok, tok)

    def gate_block(b, _):
        at = lanes(b)
        held = [starts[b * per_block + p].astype(F32) for p in range(per_block)]
        totals = [local[t * SUB:(t + 1) * SUB, at] for t in range(tiles)]
        for m in range(modes):
            rate = rate_ref[pl.ds(m, 1), at]
            jump = jnp.exp(-float(SUB) * rate)
            start = held[m // rows][m % rows:m % rows + 1]
            term = (amp_ref[pl.ds(m, 1), at] * start) * jnp.exp(-rate * (steps + 1.0))
            for t in range(tiles):
                totals[t] = totals[t] + term
                if t < tiles - 1:
                    term = term * jump
        gated = q_ref[:, at].astype(F32) * jnp.concatenate(totals, axis=0)
        gathered[pl.ds(own_rows, tok), at] = gated.astype(BF16)
        return 0


    half_cols = chans // 2
    sib = me + 1 - 2 * c
    has_right = z < line - 1
    has_left = z > 0
    sent = []

    def piece(half, slot):
        return gathered.at[
            pl.ds(pl.multiple_of(slot * tok, tok), tok), pl.ds(half * half_cols, half_cols)
        ]

    def send(half, slot, peer, cond):
        copy = pltpu.make_async_remote_copy(
            src_ref=piece(half, slot), dst_ref=piece(half, slot),
            send_sem=gather_send.at[len(sent)], recv_sem=gather_recv.at[half * 2 * line + slot],
            device_id=(peer, chan), device_id_type=MESH,
        )
        sent.append((cond, copy))
        pl.when(cond)(copy.start)

    def receive(half, slot):
        pltpu.make_async_remote_copy(
            src_ref=piece(half, slot), dst_ref=piece(half, slot),
            send_sem=gather_send.at[0], recv_sem=gather_recv.at[half * 2 * line + slot],
            device_id=(sib, chan), device_id_type=MESH,
        ).wait_recv()

    out_chan = me // per_chan

    def part_copy(other, zz, to_core):
        to = zz * 4 + x * 2 + to_core
        owner = across if other else me
        slot = 2 * zz + to_core
        place = chan * per_chan + lax.rem(owner, per_chan)
        source = partial.at[
            pl.ds(pl.multiple_of((other * 2 * line + slot) * tok, tok), tok)
        ]
        remote = pltpu.make_async_remote_copy(
            src_ref=source, dst_ref=landed.at[place],
            send_sem=part_send.at[other * 2 * line + slot], recv_sem=part_recv.at[place],
            device_id=(to, out_chan), device_id_type=MESH,
        )
        here = pltpu.make_async_copy(source, landed.at[place], part_recv.at[place])
        return to, remote, here

    def project(zz, other):
        at = pl.ds(pl.multiple_of(zz * 2 * tok, 2 * tok), 2 * tok)
        to_rows = pl.ds(pl.multiple_of((other * line + zz) * 2 * tok, 2 * tok), 2 * tok)
        weights = w_other if other else w_ref
        partial[to_rows] = jnp.dot(
            gathered[at], weights[...], preferred_element_type=F32
        ).astype(BF16)
        for to_core in range(2):
            to, remote, here = part_copy(other, zz, to_core)
            stays = jnp.logical_and(to == me, out_chan == chan)
            pl.when(stays)(here.start)
            pl.when(jnp.logical_not(stays))(remote.start)

    for half in range(2):
        lax.fori_loop(half * blocks // 2, (half + 1) * blocks // 2, gate_block, 0)
        send(half, 2 * z + c, me + 4, has_right)
        send(half, 2 * z + c, me - 4, has_left)
        send(half, 2 * z + c, sib, z >= 0)
    loads[5].wait()
    for half in range(2):
        receive(half, 2 * z + 1 - c)
    project(z, 0)

    def others(last):
        for copy in w_copies:
            copy.wait_recv()
        project(z, 1)
        for d in range(1, last):
            for sign in (-1, 1):
                zz = z + sign * d
                there = zz >= 0 if sign < 0 else zz < line

                @pl.when(there)
                def _():
                    project(zz, 1)

    for d in range(1, line):
        if d == line - 1:
            others(d)
        for half in range(2):
            for sign in (-1, 1):
                zz = z + sign * d
                there = zz >= 0 if sign < 0 else zz < line
                onward = has_right if sign < 0 else has_left
                slot = 2 * zz + c

                @pl.when(there)
                def _():
                    receive(half, slot)

                send(half, slot, me - 4 * sign, jnp.logical_and(there, onward))
                send(half, slot, sib, there)
        for sign in (-1, 1):
            zz = z + sign * d
            there = zz >= 0 if sign < 0 else zz < line

            @pl.when(there)
            def _():
                for half in range(2):
                    receive(half, 2 * zz + 1 - c)
                project(zz, 0)
                if d == line - 1:
                    project(zz, 1)
    if line == 1:
        others(1)

    for i in range(per_chan):
        total = None
        for j in range(n_chan):
            slot = j * per_chan + i
            pltpu.make_async_remote_copy(
                src_ref=landed.at[slot], dst_ref=landed.at[slot],
                send_sem=part_send.at[0], recv_sem=part_recv.at[slot],
                device_id=(sib, chan), device_id_type=MESH,
            ).wait_recv()
            part = landed[slot].astype(F32)
            total = part if total is None else total + part
        out_ref[:, i * width:(i + 1) * width] = total.astype(BF16)

    for copy in end_copies + start_copies + w_copies:
        copy.wait_send()
    for cond, copy in sent:
        pl.when(cond)(copy.wait_send)
    for other in range(2):
        for slot in range(2 * line):
            to, remote, _ = part_copy(other, slot // 2, slot % 2)
            stays = jnp.logical_and(to == me, out_chan == chan)
            pl.when(jnp.logical_not(stays))(remote.wait_send)


def solution(mesh):
    n, n_chan = mesh.shape["seq"], mesh.shape["chan"]
    assert n % 4 == 0 and n % (4 * n_chan) == 0

    def body(gate_input, key_input, value_input, decay_rate, residue, skip_gain, out_weight):
        tok, chans = gate_input.shape
        modes = decay_rate.shape[0]
        width = out_weight.shape[1]
        rows = modes * chans // (LANES * n)
        hbm = pl.BlockSpec(memory_space=pltpu.HBM)
        vmem = pl.BlockSpec(memory_space=pltpu.VMEM)
        dma = pltpu.SemaphoreType.DMA
        states = pltpu.VMEM((n, rows, LANES), BF16)
        return pl.pallas_call(
            functools.partial(kernel, n, n_chan),
            out_shape=jax.ShapeDtypeStruct((tok, width * (n // n_chan)), BF16),
            in_specs=[hbm] * 5 + [vmem, hbm],
            out_specs=vmem,
            scratch_shapes=[
                pltpu.VMEM((tok, chans), BF16),
                pltpu.VMEM((tok, chans), BF16),
                pltpu.VMEM((tok, chans), BF16),
                pltpu.VMEM((modes, chans), F32),
                pltpu.VMEM((modes, chans), F32),
                pltpu.VMEM((chans, width), BF16),
                pltpu.VMEM((chans, width), BF16),
                dma((6,)), dma((8,)), dma((8,)),
                pltpu.VMEM((tok, chans), F32),
                pltpu.VMEM((tok, chans), F32),
                pltpu.VMEM((tok + SUB, LANES), F32),
                pltpu.VMEM((n, rows, LANES), F32),
                states, states, states, states,
                pltpu.VMEM((n * tok // 2, chans), BF16),
                pltpu.VMEM((n * tok, width), BF16),
                pltpu.VMEM((n, tok, width), BF16),
                dma((n,)), dma((n,)), dma((n,)), dma((n,)),
                dma((2 * n,)), dma((n,)), dma((n,)), dma((n,)),
            ],
            compiler_params=pltpu.CompilerParams(
                collective_id=0, has_side_effects=True, vmem_limit_bytes=67043328
            ),
            cost_estimate=pl.CostEstimate(
                flops=2 * n * tok * chans * width, bytes_accessed=4 * tok * chans, transcendentals=0
            ),
        )(gate_input, key_input, value_input, decay_rate, residue,
          skip_gain.reshape(1, chans), out_weight)

    return jax.shard_map(
        body,
        mesh=mesh,
        in_specs=(
            P("seq", "chan"),
            P("seq", "chan"),
            P("seq", "chan"),
            P(None, "chan"),
            P(None, "chan"),
            P("chan"),
            P("chan", "seq"),
        ),
        out_specs=P("seq", "chan"),
        check_vma=False,
    )
```
